32 devices in a mesh: rep: 4 (over x, core), shard: 8 (over z, y).
Axes of the slice: x: 2, y: 2, z: 4, core: 2. Of those that a mesh axis runs over, the one named last changes fastest.
Arguments:
- x_in: bfloat16 [32, 512, 1024], P(('rep', 'shard')), may hold values from -6 to 6
- ln1_gain: bfloat16 [1024], P('shard'), may hold values from 0.25 to 1.75
- ln1_bias: bfloat16 [1024], P('shard'), may hold values from -1.75 to 1.75
- w_qkv: bfloat16 [1024, 3072], P('shard'), may hold values from -0.25 to 0.25
- b_qv: bfloat16 [2048], P('shard'), may hold values from -1.75 to 1.75
- w_out: bfloat16 [1024, 1024], P('shard'), may hold values from -1 to 1
- b_out: bfloat16 [1024], P('shard'), may hold values from -1.75 to 1.75
- ln2_gain: bfloat16 [1024], P('shard'), may hold values from 0.25 to 1.75
- ln2_bias: bfloat16 [1024], P('shard'), may hold values from -1.75 to 1.75
- w_up: bfloat16 [1024, 4096], P('shard'), may hold values from -0.1875 to 0.1875
- b_up: bfloat16 [4096], P('shard'), may hold values from -3 to 3
- w_down: bfloat16 [4096, 1024], P('shard'), may hold values from -0.09375 to 0.09375
- b_down: bfloat16 [1024], P('shard'), may hold values from -1.75 to 1.75
- cotangent: bfloat16 [32, 512, 1024], P(('rep', 'shard')), may hold values from -6 to 6
Outputs:
- output: bfloat16 [32, 512, 1024], P(('rep', 'shard'))
- grad_input: bfloat16 [32, 512, 1024], P(('rep', 'shard'))
- grad_ln1_gain: float32 [1024], P('shard')
- grad_ln1_bias: float32 [1024], P('shard')
- grad_w_qkv: float32 [1024, 3072], P('shard')
- grad_b_qv: float32 [2048], P('shard')
- grad_w_out: float32 [1024, 1024], P('shard')
- grad_b_out: float32 [1024], P('shard')
- grad_ln2_gain: float32 [1024], P('shard')
- grad_ln2_bias: float32 [1024], P('shard')
- grad_w_up: float32 [1024, 4096], P('shard')
- grad_b_up: float32 [4096], P('shard')
- grad_w_down: float32 [4096, 1024], P('shard')
- grad_b_down: float32 [1024], P('shard')
The draws below stay inside these ranges and needn't reach their ends.
All inputs are finite; a program needn't handle non-finite values.
Results may differ from the reference program's by a relative error of at most 0.015.
Values may be sent and summed in bfloat16 or wider, within the bound.
A program may use at most 192 MiB of HBM per device.

```python
import math
import jax
import jax.numpy as jnp
from jax import lax

D = 1024
HEADS = 16
HEAD_DIM = 64
FF = 4096
SEQ = 512
IMAGES = 32


def levels(key, shape, cuts, smallest, largest):
    factor_of, own = 1.0, jax.random.fold_in(key, 6)
    for axis_at, parts in cuts:
        draws = jnp.exp(jax.random.uniform(jax.random.fold_in(own, axis_at), (parts,), jnp.float32, smallest / len(cuts), largest / len(cuts)))
        factor_of = factor_of * jnp.repeat(draws, shape[axis_at] // parts).reshape([-1 if axis == axis_at else 1 for axis in range(len(shape))])
    return factor_of


def noise(key, extent, width, bound, cuts=(), held_as=jnp.bfloat16):
    factor_of = levels(key, extent, cuts, -0.22, 0.18) if cuts else 1.0
    array = jax.random.normal(key, extent, jnp.float32) * width * factor_of
    return jnp.minimum(jnp.maximum(array, -bound), bound).astype(held_as)


def setup_inputs(seed: int = 0) -> dict:
    arg_keys = jax.random.split(jax.random.key(seed), 15)
    x_in = noise(arg_keys[0], (IMAGES, SEQ, D), 1.0, 6.0, ((0, 32),))
    ln1_gain = jnp.clip(1.0 + 0.15 * jax.random.normal(arg_keys[1], (D,), jnp.float32), 0.25, 1.75).astype(jnp.bfloat16)
    ln1_bias = noise(arg_keys[2], (D,), 0.3, 1.75, ((0, 8),))
    w_qkv = noise(arg_keys[3], (D, 3 * D), (D // 2) ** -0.5, 0.25, ((0, 8),))
    b_qv = noise(arg_keys[4], (2 * D,), 0.3, 1.75, ((0, 8),))
    w_out = noise(arg_keys[5], (D, D), (D // 32) ** -0.5, 1.0, ((0, 8),))
    b_out = noise(arg_keys[6], (D,), 0.3, 1.75, ((0, 8),))
    ln2_gain = jnp.clip(1.0 + 0.15 * jax.random.normal(arg_keys[7], (D,), jnp.float32), 0.25, 1.75).astype(jnp.bfloat16)
    ln2_bias = noise(arg_keys[8], (D,), 0.3, 1.75, ((0, 8),))
    w_up = noise(arg_keys[9], (D, FF), D ** -0.5, 0.1875, ((0, 8),))
    b_up = noise(arg_keys[10], (FF,), 0.5, 3.0, ((0, 8),))
    w_down = noise(arg_keys[11], (FF, D), FF ** -0.5, 0.09375, ((0, 8),))
    b_down = noise(arg_keys[12], (D,), 0.3, 1.75, ((0, 8),))
    cotangent = noise(arg_keys[13], (IMAGES, SEQ, D), 1.0, 6.0, ((0, 32),))
    return {"x_in": x_in, "ln1_gain": ln1_gain, "ln1_bias": ln1_bias, "w_qkv": w_qkv, "b_qv": b_qv, "w_out": w_out, "b_out": b_out, "ln2_gain": ln2_gain, "ln2_bias": ln2_bias, "w_up": w_up, "b_up": b_up, "w_down": w_down, "b_down": b_down, "cotangent": cotangent}


EPSILON = 1e-06
EXACT_PRECISION = lax.Precision.HIGHEST

@jax.custom_vjp
def low(v):
    return lax.optimization_barrier(v.astype(jnp.bfloat16)).astype(jnp.float32)

@jax.custom_vjp
def reduced_backward(v):
    return v

def low_keep(v):
    return (low(v), None)

def low_pass(kept, grad):
    return (grad,)

def back_keep(v):
    return (v, None)

def back_low(kept, grad):
    return (low(grad),)
low.defvjp(low_keep, low_pass)
reduced_backward.defvjp(back_keep, back_low)

def layer_norm(values, gain_vec, shift_vec):
    center = values - lax.optimization_barrier(jnp.mean(values, axis=-1, keepdims=True))
    spread = lax.optimization_barrier(jnp.mean(center * center, axis=-1, keepdims=True))
    return center * lax.rsqrt(spread + EPSILON) * gain_vec + shift_vec

def gelu_exact(values):
    return jax.nn.gelu(values, approximate=False)

def head_attend(head_triple):
    query_matrix, key_matrix, value_matrix = head_triple
    logit_scale_factor = 1.0 / math.sqrt(HEAD_DIM)
    attention_scores = reduced_backward(jnp.einsum('ugs,uxs->ugx', query_matrix, key_matrix, precision=EXACT_PRECISION) * logit_scale_factor)
    weight_params = low(jax.nn.softmax(attention_scores, axis=-1))
    return jnp.einsum('oaw,owy->oay', weight_params, value_matrix, precision=EXACT_PRECISION)

def forward(x_rows, ln1_gain, ln1_bias, w_qkv, b_qv, w_out, b_out, ln2_gain, ln2_bias, w_up, b_up, w_down, b_down):
    batch_size = x_rows.shape[0]
    normed = low(layer_norm(x_rows, ln1_gain, ln1_bias))
    bias_all = jnp.concatenate([b_qv[:D], jnp.zeros((D,), jnp.float32), b_qv[D:]])
    projected = reduced_backward(low(jnp.einsum('bsd,de->bse', normed, w_qkv, precision=EXACT_PRECISION) + bias_all))

    def to_heads(columns):
        return columns.reshape(batch_size, SEQ, HEADS, HEAD_DIM).transpose(2, 0, 1, 3)
    attended = lax.map(jax.checkpoint(head_attend), (to_heads(projected[..., :D]), to_heads(projected[..., D:2 * D]), to_heads(projected[..., 2 * D:])))
    context = reduced_backward(low(attended.transpose(1, 2, 0, 3).reshape(batch_size, SEQ, D)))
    branch = reduced_backward(jnp.einsum('bsd,de->bse', context, w_out, precision=EXACT_PRECISION) + b_out)
    middle = x_rows + branch
    normed_two = low(layer_norm(middle, ln2_gain, ln2_bias))
    hidden = reduced_backward(jnp.einsum('bsd,df->bsf', normed_two, w_up, precision=EXACT_PRECISION) + b_up)
    active = low(gelu_exact(hidden))
    result = reduced_backward(jnp.einsum('bsf,fd->bsd', active, w_down, precision=EXACT_PRECISION) + b_down)
    return middle + result

def reference(x_in, ln1_gain, ln1_bias, w_qkv, b_qv, w_out, b_out, ln2_gain, ln2_bias, w_up, b_up, w_down, b_down, cotangent):
    weights_wide = tuple((weight_item.astype(jnp.float32) for weight_item in (ln1_gain, ln1_bias, w_qkv, b_qv, w_out, b_out, ln2_gain, ln2_bias, w_up, b_up, w_down, b_down)))
    group_count = IMAGES // 8
    image_rows = x_in.astype(jnp.float32).reshape(group_count, 8, SEQ, D)
    cot_rows = cotangent.astype(jnp.float32).reshape(group_count, 8, SEQ, D)

    def accumulate(totals, image_pair):
        image_block, grad_block = image_pair
        result, pullback = jax.vjp(forward, image_block, *weights_wide)
        all_grads = pullback(grad_block)
        totals = tuple((grad_total + one_grad for grad_total, one_grad in zip(totals, all_grads[1:])))
        return (totals, (result.astype(jnp.bfloat16), all_grads[0].astype(jnp.bfloat16)))
    zero_sums = tuple((jnp.zeros_like(weight_item) for weight_item in weights_wide))
    totals, (outputs, input_grads) = lax.scan(accumulate, zero_sums, (image_rows, cot_rows))
    return (outputs.reshape(IMAGES, SEQ, D), input_grads.reshape(IMAGES, SEQ, D), totals[0], totals[1], totals[2], totals[3], totals[4], totals[5], totals[6], totals[7], totals[8], totals[9], totals[10], totals[11])
```

```python
import functools
import math

import jax
import jax.numpy as jnp
from jax import lax
from jax.experimental import pallas as pl
from jax.experimental.pallas import tpu as pltpu
from jax.sharding import PartitionSpec as P

HEADS = 16
HEAD_DIM = 64
EPSILON = 1e-06
MESH = pl.DeviceIdType.MESH
F32 = jnp.float32
BF16 = jnp.bfloat16
PIECES = 8


def nt(a, b):
    return lax.dot_general(a, b, (((1,), (1,)), ((), ())), preferred_element_type=F32)


def nn(a, b):
    return lax.dot_general(a, b, (((1,), (0,)), ((), ())), preferred_element_type=F32)


def tn(a, b):
    return lax.dot_general(a, b, (((0,), (0,)), ((), ())), preferred_element_type=F32)


def softmax_rows(q, k):
    scores = nt(q, k) * (1.0 / math.sqrt(HEAD_DIM))
    peak = jnp.max(scores, axis=-1, keepdims=True)
    grown = jnp.exp(scores - peak)
    return grown / jnp.sum(grown, axis=-1, keepdims=True)


def attend_kernel(q_ref, k_ref, v_ref, o_ref):
    q, k, v = q_ref[...], k_ref[...], v_ref[...]
    parts = []
    for j in range(2):
        cols = slice(j * HEAD_DIM, (j + 1) * HEAD_DIM)
        probs = softmax_rows(q[:, cols], k[:, cols])
        parts.append(nn(probs.astype(BF16), v[:, cols]))
    o_ref[...] = jnp.concatenate(parts, axis=1).astype(BF16)


def attend_back_kernel(q_ref, k_ref, v_ref, g_ref, dq_ref, dk_ref, dv_ref):
    q, k, v, g = q_ref[...], k_ref[...], v_ref[...], g_ref[...]
    scale = 1.0 / math.sqrt(HEAD_DIM)
    dqs, dks, dvs = [], [], []
    for j in range(2):
        cols = slice(j * HEAD_DIM, (j + 1) * HEAD_DIM)
        qj, kj, vj, gj = q[:, cols], k[:, cols], v[:, cols], g[:, cols]
        probs = softmax_rows(qj, kj)
        grad_probs = nt(gj, vj)
        inner = jnp.sum(grad_probs * probs, axis=-1, keepdims=True)
        grad_scores = (probs * (grad_probs - inner)).astype(BF16)
        dqs.append(nn(grad_scores, kj) * scale)
        dks.append(tn(grad_scores, qj) * scale)
        dvs.append(tn(probs.astype(BF16), gj))
    dq_ref[...] = jnp.concatenate(dqs, axis=1).astype(BF16)
    dk_ref[...] = jnp.concatenate(dks, axis=1).astype(BF16)
    dv_ref[...] = jnp.concatenate(dvs, axis=1).astype(BF16)


def attend(projected, images, seq):
    width = projected.shape[1] // 3
    pairs = width // 128
    spec = lambda off: pl.BlockSpec((seq, 128), lambda i, h: (i, off * pairs + h))
    return pl.pallas_call(
        attend_kernel,
        grid=(images, pairs),
        in_specs=[spec(0), spec(1), spec(2)],
        out_specs=spec(0),
        out_shape=jax.ShapeDtypeStruct((images * seq, width), BF16),
    )(projected, projected, projected)


def attend_back(projected, grad_context, images, seq):
    width = projected.shape[1] // 3
    pairs = width // 128
    spec = lambda off: pl.BlockSpec((seq, 128), lambda i, h: (i, off * pairs + h))
    shape = jax.ShapeDtypeStruct((images * seq, width), BF16)
    return pl.pallas_call(
        attend_back_kernel,
        grid=(images, pairs),
        in_specs=[spec(0), spec(1), spec(2), spec(0)],
        out_specs=[spec(0), spec(0), spec(0)],
        out_shape=[shape, shape, shape],
    )(projected, projected, projected, grad_context)


class Place:
    def __init__(self, rep, shard):
        r, s = lax.axis_index("rep"), lax.axis_index("shard")
        self.rep, self.shard, self.line = rep, shard, shard // 2
        self.r, self.s = r, s
        self.x, self.c = r // 2, lax.rem(r, 2)
        self.z, self.y = s // 2, lax.rem(s, 2)
        self.x_peer = ((1 - self.x) * 2 + self.c, s)
        self.c_peer = (self.x * 2 + 1 - self.c, s)
        self.y_peer = (r, self.z * 2 + 1 - self.y)

    def piece(self, half):
        return (self.c * 2 + half) * 2 + self.x

    def z_to(self, j):
        return lax.rem(self.z + j, self.line)

    def z_from(self, j):
        return lax.rem(self.z + self.line - j, self.line)

    def z_peer(self, j):
        return (self.r, self.z_to(j) * 2 + self.y)

    def s_to(self, j):
        return lax.rem(self.s + j, self.shard)

    def s_from(self, j):
        return lax.rem(self.s + self.shard - j, self.shard)

    def r_to(self, j):
        return lax.rem(self.r + j, self.rep)

    def r_from(self, j):
        return lax.rem(self.r + self.rep - j, self.rep)

    def greet(self):
        barrier = pltpu.get_barrier_semaphore()

        def shard_signal(j, carry):
            pl.semaphore_signal(
                barrier, inc=1, device_id=(self.r, self.s_to(j)), device_id_type=MESH
            )
            return carry

        lax.fori_loop(1, self.shard, shard_signal, 0)
        for j in range(1, self.rep):
            pl.semaphore_signal(
                barrier, inc=1, device_id=(self.r_to(j), self.s), device_id_type=MESH
            )
        pl.semaphore_wait(barrier, self.shard - 1 + self.rep - 1)


def remote(src, dst, send, recv, peer):
    return pltpu.make_async_remote_copy(
        src_ref=src, dst_ref=dst, send_sem=send, recv_sem=recv, device_id=peer, device_id_type=MESH
    )


def gather_kernel(rep, shard, count, *refs):
    ins, vec = refs[:count], refs[count]
    outs, vec_out = refs[count + 1 : 2 * count + 1], refs[2 * count + 1]
    rest = refs[2 * count + 2 :]
    stages, (local_sem, near_send, near_recv, far_send, far_recv, vec_send, vec_recv) = (
        rest[: count + 1],
        rest[count + 1 :],
    )
    at = Place(rep, shard)
    line = at.line
    chunks = [(w, h) for w in range(count) for h in range(2)]

    loads = []
    for n, (w, h) in enumerate(chunks):
        load = pltpu.make_async_copy(ins[w].at[at.piece(h)], stages[w].at[h], local_sem.at[n])
        load.start()
        loads.append(load)
    vec_load = pltpu.make_async_copy(vec, stages[count], local_sem.at[len(chunks)])
    vec_load.start()

    at.greet()

    def vec_copy(j):
        return remote(
            vec,
            vec_out.at[at.s],
            vec_send.at[j - 1],
            vec_recv.at[j - 1],
            (at.r, at.s_to(j)),
        )

    def vec_start(j, carry):
        vec_copy(j).start()
        return carry

    lax.fori_loop(1, shard, vec_start, 0)

    def first(n, w, h, j):
        k = at.piece(h)
        return remote(
            ins[w].at[k],
            outs[w].at[at.z, at.y, k],
            near_send.at[n, j - 1],
            near_recv.at[n, j - 1],
            at.z_peer(j),
        )

    for n, (w, h) in enumerate(chunks):

        def start(j, carry, n=n, w=w, h=h):
            first(n, w, h, j).start()
            return carry

        lax.fori_loop(1, line, start, 0)

    stores = []
    for n, (w, h) in enumerate(chunks):
        loads[n].wait()
        store = pltpu.make_async_copy(
            stages[w].at[h], outs[w].at[at.z, at.y, at.piece(h)], local_sem.at[n]
        )
        store.start()
        stores.append(store)
    vec_load.wait()
    vec_store = pltpu.make_async_copy(stages[count], vec_out.at[at.s], local_sem.at[len(chunks)])
    vec_store.start()

    def far(n, w, h, stage):
        base = (at.c * 2 + h) * 2
        full = outs[w]
        if stage == 2:
            ref, peer = full.at[:, :, pl.ds(base, 2)], at.c_peer
        elif h == 0:
            ref, peer = (
                (full.at[:, at.y, base + at.x], at.y_peer)
                if stage == 0
                else (full.at[:, :, base + at.x], at.x_peer)
            )
        else:
            ref, peer = (
                (full.at[:, at.y, base + at.x], at.x_peer)
                if stage == 0
                else (full.at[:, at.y, pl.ds(base, 2)], at.y_peer)
            )
        return remote(ref, ref, far_send.at[n, stage], far_recv.at[n, stage], peer)

    total = len(chunks)
    for step in range(total + 3):
        for stage in range(4):
            n = step - stage
            if not 0 <= n < total:
                continue
            w, h = chunks[n]
            if stage == 0:
                stores[n].wait()

                def wait(j, carry, n=n, w=w, h=h):
                    k = at.piece(h)
                    landed = outs[w].at[at.z_from(j), at.y, k]
                    remote(
                        ins[w].at[k],
                        landed,
                        near_send.at[n, j - 1],
                        near_recv.at[n, j - 1],
                        at.z_peer(j),
                    ).wait()
                    return carry

                lax.fori_loop(1, line, wait, 0)
                far(n, w, h, 0).start()
            else:
                far(n, w, h, stage - 1).wait()
                if stage < 3:
                    far(n, w, h, stage).start()

    vec_store.wait()

    def vec_wait(j, carry):
        remote(
            vec,
            vec_out.at[at.s_from(j)],
            vec_send.at[j - 1],
            vec_recv.at[j - 1],
            (at.r, at.s_to(j)),
        ).wait()
        return carry

    lax.fori_loop(1, shard, vec_wait, 0)


def gather(rep, shard, weights, vec):
    count = len(weights)
    line = shard // 2
    cut = [w.reshape(PIECES, w.shape[0] // PIECES, w.shape[1]) for w in weights]
    chunks = 2 * count
    anywhere = pl.BlockSpec(memory_space=pl.ANY)
    results = pl.pallas_call(
        functools.partial(gather_kernel, rep, shard, count),
        in_specs=[anywhere] * (count + 1),
        out_specs=[anywhere] * (count + 1),
        out_shape=[jax.ShapeDtypeStruct((line, 2) + w.shape, w.dtype) for w in cut]
        + [jax.ShapeDtypeStruct((shard,) + vec.shape, vec.dtype)],
        scratch_shapes=[pltpu.VMEM((2,) + w.shape[1:], w.dtype) for w in cut]
        + [
            pltpu.VMEM(vec.shape, vec.dtype),
            pltpu.SemaphoreType.DMA((chunks + 1,)),
            pltpu.SemaphoreType.DMA((chunks, line - 1)),
            pltpu.SemaphoreType.DMA((chunks, line - 1)),
            pltpu.SemaphoreType.DMA((chunks, 3)),
            pltpu.SemaphoreType.DMA((chunks, 3)),
            pltpu.SemaphoreType.DMA((shard - 1,)),
            pltpu.SemaphoreType.DMA((shard - 1,)),
        ],
        compiler_params=pltpu.CompilerParams(collective_id=0, has_side_effects=True),
    )(*cut, vec)
    return [
        full.reshape(shard * w.shape[0], w.shape[1]) for full, w in zip(results[:-1], weights)
    ] + [results[-1]]


def add_blocks(grid, spec_a, spec_b, spec_out, a, b, out):
    def step(a_ref, b_ref, o_ref):
        o_ref[...] = (a_ref[...].astype(F32) + b_ref[...].astype(F32)).astype(BF16).reshape(
            o_ref.shape
        )

    pltpu.emit_pipeline(step, grid=grid, in_specs=[spec_a, spec_b], out_specs=[spec_out])(
        a, b, out
    )


def reduce_kernel(rep, shard, count, *refs):
    grads, vec = refs[:count], refs[count]
    refs = refs[count + 1 :]
    fins, vec_out = refs[:count], refs[count]
    refs = refs[count + 1 :]
    names = ("got1", "sum1", "got20", "got21", "sum20", "sum21", "got3", "sum3", "got4")
    bufs = [
        dict(zip(names, refs[i * len(names) : (i + 1) * len(names)])) for i in range(count)
    ]
    refs = refs[count * len(names) :]
    vec_got, vec_rep, vec_sum = refs[:3]
    (
        send,
        recv,
        z_send,
        z_recv,
        v_send,
        v_recv,
        r_send,
        r_recv,
        local_sem,
    ) = refs[3:12]
    vec_v = refs[12:]
    at = Place(rep, shard)
    line = at.line
    at.greet()

    def vec_copy(j):
        return remote(
            vec.at[at.s_to(j)],
            vec_got.at[at.s],
            v_send.at[j - 1],
            v_recv.at[j - 1],
            (at.r, at.s_to(j)),
        )

    def core_copy(w):
        return remote(
            grads[w].at[:, :, pl.ds((1 - at.c) * 4, 4)],
            bufs[w]["got1"],
            send.at[w, 0, 0],
            recv.at[w, 0, 0],
            at.c_peer,
        )

    def copy2(w, h):
        b = bufs[w]
        if h == 0:
            return remote(
                b["sum1"].at[:, :, 1 - at.x],
                b["got20"],
                send.at[w, 1, 0],
                recv.at[w, 1, 0],
                at.x_peer,
            )
        return remote(
            b["sum1"].at[:, 1 - at.y, pl.ds(2, 2)],
            b["got21"],
            send.at[w, 1, 1],
            recv.at[w, 1, 1],
            at.y_peer,
        )

    def copy3(w, h):
        b = bufs[w]
        src, peer = (
            (b["sum20"].at[:, 1 - at.y], at.y_peer)
            if h == 0
            else (b["sum21"].at[:, 1 - at.x], at.x_peer)
        )
        return remote(src, b["got3"].at[h], send.at[w, 2, h], recv.at[w, 2, h], peer)

    def copy4(w, h, j):
        b = bufs[w]
        return remote(
            b["sum3"].at[h, at.z_to(j)],
            b["got4"].at[h, j - 1],
            z_send.at[w, h, j - 1],
            z_recv.at[w, h, j - 1],
            at.z_peer(j),
        )

    def copy5(w, h):
        ref = fins[w].at[at.piece(h)]
        return remote(ref, ref, send.at[w, 3, h], recv.at[w, 3, h], at.x_peer)

    def landed5(w, h):
        ref = fins[w].at[(at.c * 2 + h) * 2 + 1 - at.x]
        return remote(fins[w].at[at.piece(h)], ref, send.at[w, 3, h], recv.at[w, 3, h], at.x_peer)

    def copy6(w, mine=True):
        src = fins[w].at[pl.ds(at.c * 4, 4)]
        dst = src if mine else fins[w].at[pl.ds((1 - at.c) * 4, 4)]
        return remote(src, dst, send.at[w, 4, 0], recv.at[w, 4, 0], at.c_peer)

    def add1(w):
        b = bufs[w]
        rows, cols = b["got1"].shape[-2:]
        block = (1, 2, 4, rows, cols)
        half = pl.BlockSpec(block, lambda a: (a, 0, 0, 0, 0))
        add_blocks(
            (line,), half, half, half, grads[w].at[:, :, pl.ds(at.c * 4, 4)], b["got1"], b["sum1"]
        )

    def add2(w, h):
        b = bufs[w]
        rows, cols = b["got1"].shape[-2:]
        spec = pl.BlockSpec((1, 2, rows, cols), lambda a: (a, 0, 0, 0))
        if h == 0:
            add_blocks(
                (line,), spec, spec, spec, b["sum1"].at[:, :, at.x], b["got20"], b["sum20"]
            )
        else:
            add_blocks(
                (line,),
                spec,
                spec,
                spec,
                b["sum1"].at[:, at.y, pl.ds(2, 2)],
                b["got21"],
                b["sum21"],
            )

    def add3(w, h):
        b = bufs[w]
        rows, cols = b["got1"].shape[-2:]
        step = 2 if line % 2 == 0 else 1
        spec = pl.BlockSpec((step, rows, cols), lambda a: (a, 0, 0))
        mine = b["sum20"].at[:, at.y] if h == 0 else b["sum21"].at[:, at.x]
        add_blocks((line // step,), spec, spec, spec, mine, b["got3"].at[h], b["sum3"].at[h])

    def add4(w, h):
        b = bufs[w]
        rows, cols = b["got1"].shape[-2:]
        spec = pl.BlockSpec((rows, cols), lambda a: (0, 0))
        got = pl.BlockSpec((line - 1, rows, cols), lambda a: (0, 0, 0))

        def step(a_ref, b_ref, o_ref):
            total = a_ref[...].astype(F32)
            for j in range(line - 1):
                total = total + b_ref[j].astype(F32)
            o_ref[...] = total.astype(BF16)

        pltpu.emit_pipeline(step, grid=(1,), in_specs=[spec, got], out_specs=[spec])(
            b["sum3"].at[h, at.z], b["got4"].at[h], fins[w].at[at.piece(h)]
        )

    for w in range(count):
        core_copy(w).start()

    def vec_start(j, carry):
        vec_copy(j).start()
        return carry

    lax.fori_loop(1, shard, vec_start, 0)

    def process(stage, w):
        if stage == 0:
            core_copy(w).wait()
            add1(w)
            for h in range(2):
                copy2(w, h).start()
        elif stage == 1:
            for h in range(2):
                copy2(w, h).wait()
                add2(w, h)
                copy3(w, h).start()
        elif stage == 2:
            for h in range(2):
                copy3(w, h).wait()
                add3(w, h)

                def start(j, carry, h=h):
                    copy4(w, h, j).start()
                    return carry

                lax.fori_loop(1, line, start, 0)
        elif stage == 3:
            for h in range(2):

                def wait(j, carry, h=h):
                    copy4(w, h, j).wait()
                    return carry

                lax.fori_loop(1, line, wait, 0)
                add4(w, h)
                copy5(w, h).start()
        elif stage == 4:
            for h in range(2):
                landed5(w, h).wait()
            copy6(w).start()
        else:
            copy6(w, mine=False).wait()

    for step in range(count + 5):
        for stage in range(6):
            w = step - stage
            if 0 <= w < count:
                process(stage, w)
        if step == 0:
            own, got_v, sum_v = vec_v
            load = pltpu.make_async_copy(vec.at[at.s], own, local_sem.at[0])
            load.start()

            def vec_wait(j, carry):
                remote(
                    vec.at[at.s_to(j)],
                    vec_got.at[at.s_from(j)],
                    v_send.at[j - 1],
                    v_recv.at[j - 1],
                    (at.r, at.s_to(j)),
                ).wait()
                return carry

            lax.fori_loop(1, shard, vec_wait, 0)
            load.wait()
            load = pltpu.make_async_copy(vec_got, got_v, local_sem.at[0])
            load.start()
            load.wait()
            total = own[...]

            def vec_add(j, total):
                return total + got_v[at.s_from(j)]

            total = lax.fori_loop(1, shard, vec_add, total)
            sum_v[...] = total
            store = pltpu.make_async_copy(sum_v, vec_sum, local_sem.at[0])
            store.start()
            store.wait()
            store = pltpu.make_async_copy(sum_v, vec_rep.at[at.r], local_sem.at[0])
            store.start()
            store.wait()
            for j in range(1, rep):
                remote(
                    vec_sum,
                    vec_rep.at[at.r],
                    r_send.at[j - 1],
                    r_recv.at[j - 1],
                    (at.r_to(j), at.s),
                ).start()
    for j in range(1, rep):
        remote(
            vec_sum,
            vec_rep.at[at.r_from(j)],
            r_send.at[j - 1],
            r_recv.at[j - 1],
            (at.r_to(j), at.s),
        ).wait()
    own, got_v, sum_v = vec_v
    for j in range(rep):
        load = pltpu.make_async_copy(vec_rep.at[j], own, local_sem.at[0])
        load.start()
        load.wait()
        sum_v[...] = own[...] if j == 0 else sum_v[...] + own[...]
    store = pltpu.make_async_copy(sum_v, vec_out, local_sem.at[0])
    store.start()
    store.wait()


def reduce(rep, shard, grads, vec):
    count = len(grads)
    line = shard // 2
    cut, out_shape, scratch = [], [], []
    for g in grads:
        rows, cols = g.shape[0] // shard // PIECES, g.shape[1]
        cut.append(g.reshape(line, 2, PIECES, rows, cols))
        out_shape.append(jax.ShapeDtypeStruct((PIECES, rows, cols), BF16))
        for lead in (
            (line, 2, 4),
            (line, 2, 4),
            (line, 2),
            (line, 2),
            (line, 2),
            (line, 2),
            (2, line),
            (2, line),
            (2, line - 1),
        ):
            scratch.append(jax.ShapeDtypeStruct(lead + (rows, cols), BF16))
    one = vec.shape[1:]
    out_shape.append(jax.ShapeDtypeStruct(one, F32))
    scratch += [
        jax.ShapeDtypeStruct((shard,) + one, F32),
        jax.ShapeDtypeStruct((rep,) + one, F32),
        jax.ShapeDtypeStruct(one, F32),
    ]
    anywhere = pl.BlockSpec(memory_space=pl.ANY)
    sems = [
        (count, 5, 2),
        (count, 5, 2),
        (count, 2, line - 1),
        (count, 2, line - 1),
        (shard - 1,),
        (shard - 1,),
        (rep - 1,),
        (rep - 1,),
        (1,),
    ]
    results = pl.pallas_call(
        functools.partial(reduce_kernel, rep, shard, count),
        in_specs=[anywhere] * (count + 1),
        out_specs=[anywhere] * (len(out_shape) + len(scratch)),
        out_shape=out_shape + scratch,
        scratch_shapes=[pltpu.SemaphoreType.DMA(s) for s in sems]
        + [
            pltpu.VMEM(one, F32),
            pltpu.VMEM((shard,) + one, F32),
            pltpu.VMEM(one, F32),
        ],
        compiler_params=pltpu.CompilerParams(collective_id=1, has_side_effects=True),
    )(*cut, vec)
    return [
        results[i].reshape(g.shape[0] // shard, g.shape[1]).astype(F32)
        for i, g in enumerate(grads)
    ] + [results[count]]


def normalize(values):
    center = values - jnp.mean(values, axis=-1, keepdims=True)
    spread = lax.rsqrt(jnp.mean(center * center, axis=-1, keepdims=True) + EPSILON)
    return center * spread, spread


def norm_back(grad, gain, normal, spread):
    scaled = grad * gain
    return spread * (
        scaled
        - jnp.mean(scaled, axis=-1, keepdims=True)
        - normal * jnp.mean(scaled * normal, axis=-1, keepdims=True)
    )


def body(
    rep,
    shard,
    x_in,
    ln1_gain,
    ln1_bias,
    w_qkv,
    b_qv,
    w_out,
    b_out,
    ln2_gain,
    ln2_bias,
    w_up,
    b_up,
    w_down,
    b_down,
    cotangent,
):
    images, seq, width = x_in.shape
    small = (ln1_gain, ln1_bias, b_qv, b_out, ln2_gain, ln2_bias, b_up, b_down)
    sizes = [v.shape[0] for v in small]
    packed = jnp.concatenate(small).astype(F32).reshape(1, -1)
    full_qkv, full_out, full_up, full_down, packed_full = gather(
        rep, shard, [w_qkv, w_out, w_up, w_down], packed
    )
    packed_full = packed_full.reshape(shard, -1)
    starts = [sum(sizes[:i]) for i in range(len(sizes))]
    g1, b1, bqv, bout, g2, b2, bup, bdown = [
        packed_full[:, a : a + n].reshape(-1) for a, n in zip(starts, sizes)
    ]

    rows = x_in.astype(F32).reshape(-1, width)
    normal_one, spread_one = normalize(rows)
    normed = (normal_one * g1 + b1).astype(BF16)
    bias_all = jnp.concatenate([bqv[:width], jnp.zeros((width,), F32), bqv[width:]])
    projected = (nn(normed, full_qkv) + bias_all).astype(BF16)
    context = attend(projected, images, seq)
    middle = rows + (nn(context, full_out) + bout)
    normal_two, spread_two = normalize(middle)
    normed_two = (normal_two * g2 + b2).astype(BF16)
    hidden = nn(normed_two, full_up) + bup
    inner = 0.5 * (1.0 + lax.erf(hidden * (1.0 / math.sqrt(2.0))))
    active = (hidden * inner).astype(BF16)
    output = middle + (nn(active, full_down) + bdown)

    grad_branch = cotangent.reshape(-1, width)
    grad_result = grad_branch.astype(F32)
    grad_w_down = tn(active, grad_branch).astype(BF16)
    grad_b_down = jnp.sum(grad_result, axis=0)
    slope = inner + hidden * (jnp.exp(-0.5 * hidden * hidden) * (1.0 / math.sqrt(2.0 * math.pi)))
    grad_hidden = (nt(grad_branch, full_down) * slope).astype(BF16)
    grad_w_up = tn(normed_two, grad_hidden).astype(BF16)
    grad_b_up = jnp.sum(grad_hidden.astype(F32), axis=0)
    grad_normed_two = nt(grad_hidden, full_up)
    grad_g2 = jnp.sum(grad_normed_two * normal_two, axis=0)
    grad_b2 = jnp.sum(grad_normed_two, axis=0)
    grad_middle = grad_result + norm_back(grad_normed_two, g2, normal_two, spread_two)
    grad_attn = grad_middle.astype(BF16)
    grad_w_out = tn(context, grad_attn).astype(BF16)
    grad_b_out = jnp.sum(grad_attn.astype(F32), axis=0)
    grad_context = nt(grad_attn, full_out).astype(BF16)
    grad_q, grad_k, grad_v = attend_back(projected, grad_context, images, seq)
    grad_projected = jnp.concatenate([grad_q, grad_k, grad_v], axis=1)
    grad_w_qkv = tn(normed, grad_projected).astype(BF16)
    grad_b_qv = jnp.concatenate(
        [jnp.sum(grad_q.astype(F32), axis=0), jnp.sum(grad_v.astype(F32), axis=0)]
    )
    grad_normed = nt(grad_projected, full_qkv)
    grad_g1 = jnp.sum(grad_normed * normal_one, axis=0)
    grad_b1 = jnp.sum(grad_normed, axis=0)
    grad_rows = grad_middle + norm_back(grad_normed, g1, normal_one, spread_one)

    small_grads = (
        grad_g1,
        grad_b1,
        grad_b_qv,
        grad_b_out,
        grad_g2,
        grad_b2,
        grad_b_up,
        grad_b_down,
    )
    packed_grads = jnp.concatenate([g.reshape(shard, -1) for g in small_grads], axis=1).reshape(
        shard, 1, -1
    )
    sum_down, sum_up, sum_out, sum_qkv, packed_sum = reduce(
        rep, shard, [grad_w_down, grad_w_up, grad_w_out, grad_w_qkv], packed_grads
    )
    packed_sum = packed_sum.reshape(-1)
    tg1, tb1, tbqv, tbout, tg2, tb2, tbup, tbdown = [
        packed_sum[a : a + n] for a, n in zip(starts, sizes)
    ]
    return (
        output.astype(BF16).reshape(x_in.shape),
        grad_rows.astype(BF16).reshape(x_in.shape),
        tg1,
        tb1,
        sum_qkv,
        tbqv,
        sum_out,
        tbout,
        tg2,
        tb2,
        sum_up,
        tbup,
        sum_down,
        tbdown,
    )


def solution(mesh):
    rows = P(("rep", "shard"), None, None)
    flat, wide = P("shard"), P("shard", None)
    in_specs = (rows, flat, flat, wide, flat, wide, flat, flat, flat, wide, flat, wide, flat, rows)
    out_specs = (rows, rows, flat, flat, wide, flat, wide, flat, flat, flat, wide, flat, wide, flat)
    run = functools.partial(body, mesh.shape["rep"], mesh.shape["shard"])
    return jax.shard_map(run, mesh=mesh, in_specs=in_specs, out_specs=out_specs, check_vma=False)
```

```python
import functools
import math

import jax
import jax.numpy as jnp
from jax import lax
from jax.experimental import pallas as pl
from jax.experimental.pallas import tpu as pltpu
from jax.sharding import PartitionSpec as P

HEADS = 16
HEAD_DIM = 64
EPSILON = 1e-06
MESH = pl.DeviceIdType.MESH
F32 = jnp.float32
BF16 = jnp.bfloat16
PIECES = 8


def nt(a, b):
    return lax.dot_general(a, b, (((1,), (1,)), ((), ())), preferred_element_type=F32)


def nn(a, b):
    return lax.dot_general(a, b, (((1,), (0,)), ((), ())), preferred_element_type=F32)


def tn(a, b):
    return lax.dot_general(a, b, (((0,), (0,)), ((), ())), preferred_element_type=F32)


def softmax_rows(q, k):
    scores = nt(q, k) * (1.0 / math.sqrt(HEAD_DIM))
    peak = jnp.max(scores, axis=-1, keepdims=True)
    grown = jnp.exp(scores - peak)
    return grown / jnp.sum(grown, axis=-1, keepdims=True)


def attend_kernel(q_ref, k_ref, v_ref, o_ref):
    q, k, v = q_ref[...], k_ref[...], v_ref[...]
    parts = []
    for j in range(2):
        cols = slice(j * HEAD_DIM, (j + 1) * HEAD_DIM)
        probs = softmax_rows(q[:, cols], k[:, cols])
        parts.append(nn(probs.astype(BF16), v[:, cols]))
    o_ref[...] = jnp.concatenate(parts, axis=1).astype(BF16)


def attend_back_kernel(q_ref, k_ref, v_ref, g_ref, dq_ref, dk_ref, dv_ref):
    q, k, v, g = q_ref[...], k_ref[...], v_ref[...], g_ref[...]
    scale = 1.0 / math.sqrt(HEAD_DIM)
    dqs, dks, dvs = [], [], []
    for j in range(2):
        cols = slice(j * HEAD_DIM, (j + 1) * HEAD_DIM)
        qj, kj, vj, gj = q[:, cols], k[:, cols], v[:, cols], g[:, cols]
        probs = softmax_rows(qj, kj)
        grad_probs = nt(gj, vj)
        inner = jnp.sum(grad_probs * probs, axis=-1, keepdims=True)
        grad_scores = (probs * (grad_probs - inner)).astype(BF16)
        dqs.append(nn(grad_scores, kj) * scale)
        dks.append(tn(grad_scores, qj) * scale)
        dvs.append(tn(probs.astype(BF16), gj))
    dq_ref[...] = jnp.concatenate(dqs, axis=1).astype(BF16)
    dk_ref[...] = jnp.concatenate(dks, axis=1).astype(BF16)
    dv_ref[...] = jnp.concatenate(dvs, axis=1).astype(BF16)


def attend(projected, images, seq):
    width = projected.shape[1] // 3
    pairs = width // 128
    spec = lambda off: pl.BlockSpec((seq, 128), lambda i, h: (i, off * pairs + h))
    return pl.pallas_call(
        attend_kernel,
        grid=(images, pairs),
        in_specs=[spec(0), spec(1), spec(2)],
        out_specs=spec(0),
        out_shape=jax.ShapeDtypeStruct((images * seq, width), BF16),
    )(projected, projected, projected)


def attend_back(projected, grad_context, images, seq):
    width = projected.shape[1] // 3
    pairs = width // 128
    spec = lambda off: pl.BlockSpec((seq, 128), lambda i, h: (i, off * pairs + h))
    shape = jax.ShapeDtypeStruct((images * seq, width), BF16)
    return pl.pallas_call(
        attend_back_kernel,
        grid=(images, pairs),
        in_specs=[spec(0), spec(1), spec(2), spec(0)],
        out_specs=[spec(0), spec(0), spec(0)],
        out_shape=[shape, shape, shape],
    )(projected, projected, projected, grad_context)


class Place:
    def __init__(self, rep, shard):
        r, s = lax.axis_index("rep"), lax.axis_index("shard")
        self.rep, self.shard, self.line = rep, shard, shard // 2
        self.r, self.s = r, s
        self.x, self.c = r // 2, lax.rem(r, 2)
        self.z, self.y = s // 2, lax.rem(s, 2)
        self.x_peer = ((1 - self.x) * 2 + self.c, s)
        self.c_peer = (self.x * 2 + 1 - self.c, s)
        self.y_peer = (r, self.z * 2 + 1 - self.y)

    def piece(self, half):
        return (self.c * 2 + half) * 2 + self.x

    def z_to(self, j):
        return lax.rem(self.z + j, self.line)

    def z_from(self, j):
        return lax.rem(self.z + self.line - j, self.line)

    def z_peer(self, j):
        return (self.r, self.z_to(j) * 2 + self.y)

    def s_to(self, j):
        return lax.rem(self.s + j, self.shard)

    def s_from(self, j):
        return lax.rem(self.s + self.shard - j, self.shard)

    def r_to(self, j):
        return lax.rem(self.r + j, self.rep)

    def r_from(self, j):
        return lax.rem(self.r + self.rep - j, self.rep)

    def greet(self):
        barrier = pltpu.get_barrier_semaphore()

        def shard_signal(j, carry):
            pl.semaphore_signal(
                barrier, inc=1, device_id=(self.r, self.s_to(j)), device_id_type=MESH
            )
            return carry

        lax.fori_loop(1, self.shard, shard_signal, 0)
        for j in range(1, self.rep):
            pl.semaphore_signal(
                barrier, inc=1, device_id=(self.r_to(j), self.s), device_id_type=MESH
            )
        pl.semaphore_wait(barrier, self.shard - 1 + self.rep - 1)


def remote(src, dst, send, recv, peer):
    return pltpu.make_async_remote_copy(
        src_ref=src, dst_ref=dst, send_sem=send, recv_sem=recv, device_id=peer, device_id_type=MESH
    )


SUB_ROWS = 16
SUB_COLS = 1024


def piece_shape(shard_rows, cols):
    if shard_rows % (PIECES * SUB_ROWS) == 0:
        return True, shard_rows // PIECES // SUB_ROWS, SUB_ROWS, cols
    return False, shard_rows // SUB_ROWS, SUB_ROWS, cols // PIECES


def to_pieces(array, shards):
    by_rows, sub, rows, cols = piece_shape(array.shape[0] // shards, array.shape[1])
    if by_rows:
        return array.reshape(shards, PIECES, sub, rows, cols)
    return array.reshape(shards, sub, rows, PIECES, cols).transpose(0, 3, 1, 2, 4)


def from_pieces(pieces, shape):
    shards = pieces.shape[0]
    if piece_shape(shape[0] // shards, shape[1])[0]:
        return pieces.reshape(shape)
    return pieces.transpose(0, 2, 3, 1, 4).reshape(shape)


def sub_chunks(shapes):
    found = []
    for w, (sub, _, cols) in enumerate(shapes):
        wide = min(cols, SUB_COLS)
        for i in range(sub):
            for start in range(0, cols, wide):
                found.append((w, i, start, wide))
    return found


def view(ref, lead, chunk):
    _, i, start, wide = chunk
    return ref.at[lead + (i, slice(None), pl.ds(start, wide))]


def gather_kernel(rep, shard, count, chunks, *refs):
    ins, vec = refs[:count], refs[count]
    outs, vec_out = refs[count + 1 : 2 * count + 1], refs[2 * count + 1]
    rest = refs[2 * count + 2 :]
    stages, vec_stage = rest[:count], rest[count]
    local_sem, near_send, near_recv, far_send, far_recv, vec_send, vec_recv = rest[count + 1 :]
    at = Place(rep, shard)
    line, total = at.line, len(chunks)

    loads = []
    for w in range(count):
        for h in range(2):
            load = pltpu.make_async_copy(
                ins[w].at[at.piece(h)], stages[w].at[h], local_sem.at[w, h]
            )
            load.start()
            loads.append(load)
    vec_load = pltpu.make_async_copy(vec, vec_stage, local_sem.at[count, 0])
    vec_load.start()

    at.greet()

    def vec_copy(j, landed):
        return remote(
            vec, vec_out.at[landed], vec_send.at[j - 1], vec_recv.at[j - 1], (at.r, at.s_to(j))
        )

    def vec_start(j, carry):
        vec_copy(j, at.s).start()
        return carry

    lax.fori_loop(1, shard, vec_start, 0)

    def first(n, h, j, z):
        chunk = chunks[n]
        k = at.piece(h)
        return remote(
            view(ins[chunk[0]], (k,), chunk),
            view(outs[chunk[0]], (z, at.y, k), chunk),
            near_send.at[n, h, j - 1],
            near_recv.at[n, h, j - 1],
            at.z_peer(j),
        )

    def near_start(n):
        def start(j, carry):
            for h in range(2):
                first(n, h, j, at.z).start()
            return carry

        lax.fori_loop(1, line, start, 0)

    def near_wait(n):
        def wait(j, carry):
            for h in range(2):
                first(n, h, j, at.z_from(j)).wait()
            return carry

        lax.fori_loop(1, line, wait, 0)

    near_start(0)
    stores = []
    for w in range(count):
        for h in range(2):
            loads[w * 2 + h].wait()
            store = pltpu.make_async_copy(
                stages[w].at[h], outs[w].at[at.z, at.y, at.piece(h)], local_sem.at[w, h]
            )
            store.start()
            stores.append(store)
    vec_load.wait()
    vec_store = pltpu.make_async_copy(vec_stage, vec_out.at[at.s], local_sem.at[count, 0])
    vec_store.start()
    for n in range(1, total):
        near_start(n)
    for store in stores:
        store.wait()
    vec_store.wait()

    def far(n, h, stage):
        chunk = chunks[n]
        base = (at.c * 2 + h) * 2
        all_of = slice(None)
        if stage == 2:
            lead, peer = (all_of, all_of, pl.ds(base, 2)), at.c_peer
        elif h == 0:
            lead, peer = (
                ((all_of, at.y, base + at.x), at.y_peer)
                if stage == 0
                else ((all_of, all_of, base + at.x), at.x_peer)
            )
        else:
            lead, peer = (
                ((all_of, at.y, base + at.x), at.x_peer)
                if stage == 0
                else ((all_of, at.y, pl.ds(base, 2)), at.y_peer)
            )
        ref = view(outs[chunk[0]], lead, chunk)
        return remote(ref, ref, far_send.at[n, h, stage], far_recv.at[n, h, stage], peer)

    skew = (0, 2, 4, 6)
    for step in range(total + skew[-1]):
        for stage in range(4):
            n = step - skew[stage]
            if not 0 <= n < total:
                continue
            if stage == 0:
                near_wait(n)
            for h in range(2):
                if stage > 0:
                    far(n, h, stage - 1).wait()
                if stage < 3:
                    far(n, h, stage).start()

    def vec_wait(j, carry):
        vec_copy(j, at.s_from(j)).wait()
        return carry

    lax.fori_loop(1, shard, vec_wait, 0)


def gather(rep, shard, weights, vec):
    count = len(weights)
    line = shard // 2
    cut = [to_pieces(w, 1)[0] for w in weights]
    chunks = sub_chunks([c.shape[1:] for c in cut])
    total = len(chunks)
    anywhere = pl.BlockSpec(memory_space=pl.ANY)
    results = pl.pallas_call(
        functools.partial(gather_kernel, rep, shard, count, chunks),
        in_specs=[anywhere] * (count + 1),
        out_specs=[anywhere] * (count + 1),
        out_shape=[jax.ShapeDtypeStruct((line, 2) + c.shape, c.dtype) for c in cut]
        + [jax.ShapeDtypeStruct((shard,) + vec.shape, vec.dtype)],
        scratch_shapes=[pltpu.VMEM((2,) + c.shape[1:], c.dtype) for c in cut]
        + [
            pltpu.VMEM(vec.shape, vec.dtype),
            pltpu.SemaphoreType.DMA((count + 1, 2)),
            pltpu.SemaphoreType.DMA((total, 2, line - 1)),
            pltpu.SemaphoreType.DMA((total, 2, line - 1)),
            pltpu.SemaphoreType.DMA((total, 2, 3)),
            pltpu.SemaphoreType.DMA((total, 2, 3)),
            pltpu.SemaphoreType.DMA((shard - 1,)),
            pltpu.SemaphoreType.DMA((shard - 1,)),
        ],
        compiler_params=pltpu.CompilerParams(collective_id=0, has_side_effects=True),
    )(*cut, vec)
    return [
        from_pieces(full.reshape((shard,) + full.shape[2:]), (shard * w.shape[0], w.shape[1]))
        for full, w in zip(results[:-1], weights)
    ] + [results[-1]]


def reduce_kernel(rep, shard, count, chunks, *refs):
    grads, vec = refs[:count], refs[count]
    refs = refs[count + 1 :]
    outs, vec_out, vec_got, vec_rep, vec_sum = refs[:count], *refs[count : count + 4]
    refs = refs[count + 4 :]
    names = ("own", "got1", "got20", "got21", "got3", "got4", "fin", "wide")
    bufs = [dict(zip(names, refs[i * len(names) : (i + 1) * len(names)])) for i in range(count)]
    refs = refs[count * len(names) :]
    send, recv, z_send, z_recv, v_send, v_recv, r_send, r_recv, own_sem, out_sem, local_sem = refs[
        :11
    ]
    own_v, got_v, sum_v = refs[11:]
    at = Place(rep, shard)
    line, total = at.line, len(chunks)
    all_of = slice(None)

    def fetch(w):
        return pltpu.make_async_copy(
            grads[w].at[:, :, pl.ds(at.c * 4, 4)], bufs[w]["own"], own_sem.at[w]
        )

    for w in range(count):
        fetch(w).start()
    at.greet()

    def sems(n, stage, h):
        return send.at[n, stage, h], recv.at[n, stage, h]

    def core_copy(n):
        chunk = chunks[n]
        return remote(
            view(grads[chunk[0]], (all_of, all_of, pl.ds((1 - at.c) * 4, 4)), chunk),
            view(bufs[chunk[0]]["got1"], (all_of, all_of, all_of), chunk),
            *sems(n, 0, 0),
            at.c_peer,
        )

    def copy2(n, h):
        chunk = chunks[n]
        b = bufs[chunk[0]]
        if h == 0:
            lead, to, peer = (all_of, all_of, 1 - at.x), "got20", at.x_peer
        else:
            lead, to, peer = (all_of, 1 - at.y, pl.ds(2, 2)), "got21", at.y_peer
        return remote(
            view(b["got1"], lead, chunk), view(b[to], (all_of, all_of), chunk), *sems(n, 1, h), peer
        )

    def copy3(n, h):
        chunk = chunks[n]
        b = bufs[chunk[0]]
        if h == 0:
            src, peer = view(b["got20"], (all_of, 1 - at.y), chunk), at.y_peer
        else:
            src, peer = view(b["got21"], (all_of, 1 - at.x), chunk), at.x_peer
        return remote(src, view(b["got3"], (h, all_of), chunk), *sems(n, 2, h), peer)

    def copy4(n, h, j):
        chunk = chunks[n]
        b = bufs[chunk[0]]
        return remote(
            view(b["got3"], (h, at.z_to(j)), chunk),
            view(b["got4"], (h, j - 1), chunk),
            z_send.at[n, h, j - 1],
            z_recv.at[n, h, j - 1],
            at.z_peer(j),
        )

    def copy5(n, h, x):
        chunk = chunks[n]
        fin = bufs[chunk[0]]["fin"]
        return remote(
            view(fin, (at.piece(h),), chunk),
            view(fin, ((at.c * 2 + h) * 2 + x,), chunk),
            *sems(n, 3, h),
            at.x_peer,
        )

    def copy6(n, c):
        chunk = chunks[n]
        fin = bufs[chunk[0]]["fin"]
        return remote(
            view(fin, (pl.ds(at.c * 4, 4),), chunk),
            view(fin, (pl.ds(c * 4, 4),), chunk),
            *sems(n, 4, 0),
            at.c_peer,
        )

    def write_out(n):
        chunk = chunks[n]
        w = chunk[0]
        return pltpu.make_async_copy(
            view(bufs[w]["wide"], (all_of,), chunk), view(outs[w], (all_of,), chunk), out_sem.at[n]
        )

    def each_line(action):
        def step(a, carry):
            action(a)
            return carry

        lax.fori_loop(0, line, step, 0)

    fetched = set()

    def process(stage, n):
        chunk = chunks[n]
        w, i, start, wide = chunk
        b = bufs[w]
        tail = (i, all_of, slice(start, start + wide))
        if stage == 0:
            if w not in fetched:
                fetch(w).wait()
                fetched.add(w)
            core_copy(n).wait()

            def add(a):
                at_ = (a, all_of, all_of) + tail
                b["got1"][at_] = b["got1"][at_] + b["own"][at_]

            each_line(add)
            for h in range(2):
                copy2(n, h).start()
        elif stage == 1:
            for h in range(2):
                copy2(n, h).wait()

                def add(a, h=h):
                    at_ = (a, all_of) + tail
                    mine = (a, all_of, at.x) if h == 0 else (a, at.y, slice(2, 4))
                    to = b["got20"] if h == 0 else b["got21"]
                    to[at_] = to[at_] + b["got1"][mine + tail]

                each_line(add)
                copy3(n, h).start()
        elif stage == 2:
            for h in range(2):
                copy3(n, h).wait()

                def add(a, h=h):
                    at_ = (h, a) + tail
                    mine = (
                        b["got20"][(a, at.y) + tail] if h == 0 else b["got21"][(a, at.x) + tail]
                    )
                    b["got3"][at_] = b["got3"][at_] + mine

                each_line(add)

                def begin(j, carry, h=h):
                    copy4(n, h, j).start()
                    return carry

                lax.fori_loop(1, line, begin, 0)
        elif stage == 3:
            for h in range(2):

                def wait(j, carry, h=h):
                    copy4(n, h, j).wait()
                    return carry

                lax.fori_loop(1, line, wait, 0)

                def add(j, carry, h=h):
                    return carry + b["got4"][(h, j) + tail].astype(F32)

                summed = lax.fori_loop(
                    0, line - 1, add, b["got3"][(h, at.z) + tail].astype(F32)
                )
                b["fin"][(at.piece(h),) + tail] = summed.astype(BF16)
                copy5(n, h, at.x).start()
        elif stage == 4:
            for h in range(2):
                copy5(n, h, 1 - at.x).wait()
            copy6(n, at.c).start()
        else:
            copy6(n, 1 - at.c).wait()

            def widen(k, carry):
                b["wide"][(k,) + tail] = b["fin"][(k,) + tail].astype(F32)
                return carry

            lax.fori_loop(0, PIECES, widen, 0)
            write_out(n).start()

    def vec_copy(j, landed):
        return remote(
            vec.at[at.s_to(j)],
            vec_got.at[landed],
            v_send.at[j - 1],
            v_recv.at[j - 1],
            (at.r, at.s_to(j)),
        )

    def vec_start(j, carry):
        vec_copy(j, at.s).start()
        return carry

    def local(src, dst):
        copy = pltpu.make_async_copy(src, dst, local_sem.at[0])
        copy.start()
        copy.wait()

    def rep_copy(j, landed):
        return remote(
            vec_sum,
            vec_rep.at[landed],
            r_send.at[j - 1],
            r_recv.at[j - 1],
            (at.r_to(j), at.s),
        )

    def small_first():
        def vec_wait(j, carry):
            vec_copy(j, at.s_from(j)).wait()
            return carry

        lax.fori_loop(1, shard, vec_wait, 0)
        local(vec.at[at.s], own_v)
        local(vec_got, got_v)

        def vec_add(j, carry):
            return carry + got_v[at.s_from(j)]

        sum_v[...] = lax.fori_loop(1, shard, vec_add, own_v[...])
        local(sum_v, vec_sum)
        local(sum_v, vec_rep.at[at.r])
        for j in range(1, rep):
            rep_copy(j, at.r).start()

    def small_last():
        for j in range(1, rep):
            rep_copy(j, at.r_from(j)).wait()
        for j in range(rep):
            local(vec_rep.at[j], own_v)
            sum_v[...] = own_v[...] if j == 0 else sum_v[...] + own_v[...]
        local(sum_v, vec_out)

    core_copy(0).start()
    lax.fori_loop(1, shard, vec_start, 0)
    for n in range(1, total):
        core_copy(n).start()

    skew = (0, 2, 4, 6, 8, 9)
    for step in range(total + skew[-1]):
        for stage in range(6):
            n = step - skew[stage]
            if 0 <= n < total:
                process(stage, n)
        if step == 4:
            small_first()
        if step == 8:
            small_last()
    for n in range(total):
        write_out(n).wait()


def reduce(rep, shard, grads, vec):
    count = len(grads)
    line = shard // 2
    cut, out_shape, scratch = [], [], []
    for g in grads:
        pieces = to_pieces(g, shard)
        tail = pieces.shape[2:]
        cut.append(pieces.reshape((line, 2) + pieces.shape[1:]))
        out_shape.append(jax.ShapeDtypeStruct((PIECES,) + tail, F32))
        for lead in (
            (line, 2, 4),
            (line, 2, 4),
            (line, 2),
            (line, 2),
            (2, line),
            (2, line - 1),
            (PIECES,),
        ):
            scratch.append(pltpu.VMEM(lead + tail, BF16))
        scratch.append(pltpu.VMEM((PIECES,) + tail, F32))
    chunks = sub_chunks([c.shape[3:] for c in cut])
    total = len(chunks)
    one = vec.shape[1:]
    out_shape += [
        jax.ShapeDtypeStruct(one, F32),
        jax.ShapeDtypeStruct((shard,) + one, F32),
        jax.ShapeDtypeStruct((rep,) + one, F32),
        jax.ShapeDtypeStruct(one, F32),
    ]
    anywhere = pl.BlockSpec(memory_space=pl.ANY)
    sems = [
        (total, 5, 2),
        (total, 5, 2),
        (total, 2, line - 1),
        (total, 2, line - 1),
        (shard - 1,),
        (shard - 1,),
        (rep - 1,),
        (rep - 1,),
        (count,),
        (total,),
        (1,),
    ]
    results = pl.pallas_call(
        functools.partial(reduce_kernel, rep, shard, count, chunks),
        in_specs=[anywhere] * (count + 1),
        out_specs=[anywhere] * len(out_shape),
        out_shape=out_shape,
        scratch_shapes=scratch
        + [pltpu.SemaphoreType.DMA(s) for s in sems]
        + [
            pltpu.VMEM(one, F32),
            pltpu.VMEM((shard,) + one, F32),
            pltpu.VMEM(one, F32),
        ],
        compiler_params=pltpu.CompilerParams(
            collective_id=1, has_side_effects=True, vmem_limit_bytes=60 * 1024 * 1024
        ),
    )(*cut, vec)
    return [
        from_pieces(results[i][None], (g.shape[0] // shard, g.shape[1]))
        for i, g in enumerate(grads)
    ] + [results[count]]


def normalize(values):
    center = values - jnp.mean(values, axis=-1, keepdims=True)
    spread = lax.rsqrt(jnp.mean(center * center, axis=-1, keepdims=True) + EPSILON)
    return center * spread, spread


def norm_back(grad, gain, normal, spread):
    scaled = grad * gain
    return spread * (
        scaled
        - jnp.mean(scaled, axis=-1, keepdims=True)
        - normal * jnp.mean(scaled * normal, axis=-1, keepdims=True)
    )


def body(
    rep,
    shard,
    x_in,
    ln1_gain,
    ln1_bias,
    w_qkv,
    b_qv,
    w_out,
    b_out,
    ln2_gain,
    ln2_bias,
    w_up,
    b_up,
    w_down,
    b_down,
    cotangent,
):
    images, seq, width = x_in.shape
    small = (ln1_gain, ln1_bias, b_qv, b_out, ln2_gain, ln2_bias, b_up, b_down)
    sizes = [v.shape[0] for v in small]
    packed = jnp.concatenate(small).astype(F32).reshape(1, -1)
    full_qkv, full_out, full_up, full_down, packed_full = gather(
        rep, shard, [w_qkv, w_out, w_up, w_down], packed
    )
    packed_full = packed_full.reshape(shard, -1)
    starts = [sum(sizes[:i]) for i in range(len(sizes))]
    g1, b1, bqv, bout, g2, b2, bup, bdown = [
        packed_full[:, a : a + n].reshape(-1) for a, n in zip(starts, sizes)
    ]

    rows = x_in.astype(F32).reshape(-1, width)
    normal_one, spread_one = normalize(rows)
    normed = (normal_one * g1 + b1).astype(BF16)
    bias_all = jnp.concatenate([bqv[:width], jnp.zeros((width,), F32), bqv[width:]])
    projected = (nn(normed, full_qkv) + bias_all).astype(BF16)
    context = attend(projected, images, seq)
    middle = rows + (nn(context, full_out) + bout)
    normal_two, spread_two = normalize(middle)
    normed_two = (normal_two * g2 + b2).astype(BF16)
    hidden = nn(normed_two, full_up) + bup
    inner = 0.5 * (1.0 + lax.erf(hidden * (1.0 / math.sqrt(2.0))))
    active = (hidden * inner).astype(BF16)
    output = middle + (nn(active, full_down) + bdown)

    grad_branch = cotangent.reshape(-1, width)
    grad_result = grad_branch.astype(F32)
    grad_w_down = tn(active, grad_branch).astype(BF16)
    grad_b_down = jnp.sum(grad_result, axis=0)
    slope = inner + hidden * (jnp.exp(-0.5 * hidden * hidden) * (1.0 / math.sqrt(2.0 * math.pi)))
    grad_hidden = (nt(grad_branch, full_down) * slope).astype(BF16)
    grad_w_up = tn(normed_two, grad_hidden).astype(BF16)
    grad_b_up = jnp.sum(grad_hidden.astype(F32), axis=0)
    grad_normed_two = nt(grad_hidden, full_up)
    grad_g2 = jnp.sum(grad_normed_two * normal_two, axis=0)
    grad_b2 = jnp.sum(grad_normed_two, axis=0)
    grad_middle = grad_result + norm_back(grad_normed_two, g2, normal_two, spread_two)
    grad_attn = grad_middle.astype(BF16)
    grad_w_out = tn(context, grad_attn).astype(BF16)
    grad_b_out = jnp.sum(grad_attn.astype(F32), axis=0)
    grad_context = nt(grad_attn, full_out).astype(BF16)
    grad_q, grad_k, grad_v = attend_back(projected, grad_context, images, seq)
    grad_projected = jnp.concatenate([grad_q, grad_k, grad_v], axis=1)
    grad_w_qkv = tn(normed, grad_projected).astype(BF16)
    grad_b_qv = jnp.concatenate(
        [jnp.sum(grad_q.astype(F32), axis=0), jnp.sum(grad_v.astype(F32), axis=0)]
    )
    grad_normed = nt(grad_projected, full_qkv)
    grad_g1 = jnp.sum(grad_normed * normal_one, axis=0)
    grad_b1 = jnp.sum(grad_normed, axis=0)
    grad_rows = grad_middle + norm_back(grad_normed, g1, normal_one, spread_one)

    small_grads = (
        grad_g1,
        grad_b1,
        grad_b_qv,
        grad_b_out,
        grad_g2,
        grad_b2,
        grad_b_up,
        grad_b_down,
    )
    packed_grads = jnp.concatenate([g.reshape(shard, -1) for g in small_grads], axis=1).reshape(
        shard, 1, -1
    )
    sum_down, sum_up, sum_out, sum_qkv, packed_sum = reduce(
        rep, shard, [grad_w_down, grad_w_up, grad_w_out, grad_w_qkv], packed_grads
    )
    packed_sum = packed_sum.reshape(-1)
    tg1, tb1, tbqv, tbout, tg2, tb2, tbup, tbdown = [
        packed_sum[a : a + n] for a, n in zip(starts, sizes)
    ]
    return (
        output.astype(BF16).reshape(x_in.shape),
        grad_rows.astype(BF16).reshape(x_in.shape),
        tg1,
        tb1,
        sum_qkv,
        tbqv,
        sum_out,
        tbout,
        tg2,
        tb2,
        sum_up,
        tbup,
        sum_down,
        tbdown,
    )


def solution(mesh):
    rows = P(("rep", "shard"), None, None)
    flat, wide = P("shard"), P("shard", None)
    in_specs = (rows, flat, flat, wide, flat, wide, flat, flat, flat, wide, flat, wide, flat, rows)
    out_specs = (rows, rows, flat, flat, wide, flat, wide, flat, flat, flat, wide, flat, wide, flat)
    run = functools.partial(body, mesh.shape["rep"], mesh.shape["shard"])
    return jax.shard_map(run, mesh=mesh, in_specs=in_specs, out_specs=out_specs, check_vma=False)
```
